32 devices in a mesh: dp: 32 (over z, y, x, core).
Axes of the slice: x: 2, y: 2, z: 4, core: 2. Of those that a mesh axis runs over, the one named last changes fastest.
Arguments:
- x_layer0: bfloat16 [512, 128, 576], P('dp')
- x_layer1: bfloat16 [512, 128, 576], P('dp')
- d_out: bfloat16 [512, 128, 576], P('dp')
- g_attn: bfloat16 [2, 576], replicated
- w_q: bfloat16 [2, 576, 9, 64], replicated
- w_k: bfloat16 [2, 576, 3, 64], replicated
- w_v: bfloat16 [2, 576, 3, 64], replicated
- w_o: bfloat16 [2, 9, 64, 576], replicated
- g_ffn: bfloat16 [2, 576], replicated
- w_gate: bfloat16 [2, 576, 1536], replicated
- w_up: bfloat16 [2, 576, 1536], replicated
- w_down: bfloat16 [2, 1536, 576], replicated
Outputs:
- output 1: bfloat16 [512, 128, 576], P('dp')
- output 2: float32 [2, 576], replicated
- output 3: float32 [2, 576, 9, 64], replicated
- output 4: float32 [2, 576, 3, 64], replicated
- output 5: float32 [2, 576, 3, 64], replicated
- output 6: float32 [2, 9, 64, 576], replicated
- output 7: float32 [2, 576], replicated
- output 8: float32 [2, 576, 1536], replicated
- output 9: float32 [2, 576, 1536], replicated
- output 10: float32 [2, 1536, 576], replicated
All inputs are finite; a program needn't handle non-finite values.
Results may differ from the reference program's by a relative error of at most 0.02.
Values sent between devices are 32-bit elements.
A program may use at most 1 GiB of HBM per device.

```python
import jax
import jax.numpy as jnp
from jax import lax

D_MODEL = 576
N_HEADS = 9
KV_HEADS = 3
HEAD_DIM = 64
FF_DIM = 1536
BATCH_DEV = 16
SEQ_LEN = 128
DP_SIZE = 32
BATCH_ALL = BATCH_DEV * DP_SIZE
KV_GROUP = N_HEADS // KV_HEADS
ATT_SCALE = HEAD_DIM ** -0.5
NORM_EPS = 1e-6
ROPE_THETA = 10000.0


def setup_inputs(seed: int = 0) -> dict:
    key_list = jax.random.split(jax.random.key(seed), 15)
    act_shape = (BATCH_ALL, SEQ_LEN, D_MODEL)

    def activation(key_val, key_scale):
        seq_scale = 0.5 + jax.random.uniform(key_list[key_scale], (BATCH_ALL, 1, 1), jnp.float32)
        return (jax.random.normal(key_list[key_val], act_shape, jnp.float32) * seq_scale).astype(jnp.bfloat16)

    def matrix(key_idx, shape_w, fan_in):
        return (jax.random.normal(key_list[key_idx], shape_w, jnp.float32) * fan_in ** -0.5).astype(jnp.bfloat16)

    def gain_vec(key_idx):
        return (1.0 + 0.3 * jax.random.normal(key_list[key_idx], (2, D_MODEL), jnp.float32)).astype(jnp.bfloat16)

    return {
        "x_layer0": activation(0, 1),
        "x_layer1": activation(2, 3),
        "d_out": activation(4, 5),
        "g_attn": gain_vec(6),
        "w_q": matrix(7, (2, D_MODEL, N_HEADS, HEAD_DIM), D_MODEL),
        "w_k": matrix(8, (2, D_MODEL, KV_HEADS, HEAD_DIM), D_MODEL),
        "w_v": matrix(9, (2, D_MODEL, KV_HEADS, HEAD_DIM), D_MODEL),
        "w_o": matrix(10, (2, N_HEADS, HEAD_DIM, D_MODEL), N_HEADS * HEAD_DIM),
        "g_ffn": gain_vec(11),
        "w_gate": matrix(12, (2, D_MODEL, FF_DIM), D_MODEL),
        "w_up": matrix(13, (2, D_MODEL, FF_DIM), D_MODEL),
        "w_down": matrix(14, (2, FF_DIM, D_MODEL), FF_DIM),
    }


def rope_tables():
    positions = jnp.arange(SEQ_LEN, dtype=jnp.float32)
    inv_freq = ROPE_THETA ** (-jnp.arange(0, HEAD_DIM, 2, dtype=jnp.float32) / HEAD_DIM)
    angles = positions[:, None] * inv_freq[None, :]
    return jnp.cos(angles), jnp.sin(angles)


def rotate(values, cos_t, sin_t):
    x_pairs = values.reshape(values.shape[:-1] + (values.shape[-1] // 2, 2))
    x_even = x_pairs[..., 0]
    x_odd = x_pairs[..., 1]
    cos_b = cos_t[:, None, :]
    sin_b = sin_t[:, None, :]
    turned = jnp.stack([x_even * cos_b - x_odd * sin_b, x_even * sin_b + x_odd * cos_b], axis=-1)
    return turned.reshape(values.shape)


def as_bf16(values):
    return values.astype(jnp.bfloat16).astype(jnp.float32)


def rms_scale(x_resid, gain):
    return x_resid * lax.rsqrt(jnp.mean(x_resid * x_resid, axis=-1, keepdims=True) + NORM_EPS) * gain


def layer_forward(x_in, params):
    g_attn, w_q, w_k, w_v, w_o, g_ffn, w_gate, w_up, w_down = params
    cos_t, sin_t = rope_tables()
    x_resid = x_in.astype(jnp.float32)
    normed = as_bf16(rms_scale(x_resid, g_attn))
    q_pre = as_bf16(jnp.einsum("bsd,dnh->bsnh", normed, w_q))
    k_pre = as_bf16(jnp.einsum("bsd,dnh->bsnh", normed, w_k))
    v_act = as_bf16(jnp.einsum("bsd,dnh->bsnh", normed, w_v))
    q_rot = as_bf16(rotate(q_pre, cos_t, sin_t)).reshape(BATCH_DEV, SEQ_LEN, KV_HEADS, KV_GROUP, HEAD_DIM)
    k_rot = as_bf16(rotate(k_pre, cos_t, sin_t))
    causal = jnp.arange(SEQ_LEN)[:, None] >= jnp.arange(SEQ_LEN)[None, :]
    scores = jnp.einsum("bskgd,btkd->bkgst", q_rot, k_rot) * ATT_SCALE
    p_attn = as_bf16(jax.nn.softmax(jnp.where(causal, scores, -1e30), axis=-1))
    attn_out = as_bf16(jnp.einsum("bkgst,btkd->bskgd", p_attn, v_act)).reshape(BATCH_DEV, SEQ_LEN, N_HEADS, HEAD_DIM)
    x_mid = as_bf16(x_resid + jnp.einsum("bsnh,nhd->bsd", attn_out, w_o))
    normed_ffn = as_bf16(rms_scale(x_mid, g_ffn))
    gate_act = as_bf16(jnp.einsum("bsd,df->bsf", normed_ffn, w_gate))
    up_act = as_bf16(jnp.einsum("bsd,df->bsf", normed_ffn, w_up))
    hidden = as_bf16(jax.nn.silu(gate_act) * up_act)
    return (x_mid + jnp.einsum("bsf,fd->bsd", hidden, w_down)).astype(jnp.bfloat16)


def layer_grads(x_in, d_out, params):
    pull_back = jax.vjp(layer_forward, x_in, params)[1]
    return pull_back(d_out)


def reference(x_layer0, x_layer1, d_out, g_attn, w_q, w_k, w_v, w_o, g_ffn, w_gate, w_up, w_down):
    weights = (g_attn, w_q, w_k, w_v, w_o, g_ffn, w_gate, w_up, w_down)
    params_low = tuple(weight[0].astype(jnp.float32) for weight in weights)
    params_top = tuple(weight[1].astype(jnp.float32) for weight in weights)
    shape_dev = (DP_SIZE, BATCH_DEV, SEQ_LEN, D_MODEL)

    def one_shard(running, shard_in):
        x_zero, x_one, d_top = shard_in
        d_mid, grads_top = layer_grads(x_one, d_top, params_top)
        d_first, grads_low = layer_grads(x_zero, d_mid, params_low)
        running = tuple(run_sum + jnp.stack([low_grad, top_grad]) for run_sum, low_grad, top_grad in zip(running, grads_low, grads_top))
        return running, d_first

    zero_grads = tuple(jnp.zeros(weight.shape, jnp.float32) for weight in weights)
    grad_sums, dx_shards = lax.scan(one_shard, zero_grads, (x_layer0.reshape(shape_dev), x_layer1.reshape(shape_dev), d_out.reshape(shape_dev)))
    dx_layer0 = dx_shards.reshape(BATCH_ALL, SEQ_LEN, D_MODEL)
    return (dx_layer0, grad_sums[0] / DP_SIZE, grad_sums[1] / DP_SIZE, grad_sums[2] / DP_SIZE, grad_sums[3] / DP_SIZE, grad_sums[4] / DP_SIZE, grad_sums[5] / DP_SIZE, grad_sums[6] / DP_SIZE, grad_sums[7] / DP_SIZE, grad_sums[8] / DP_SIZE)
```

```python
import functools

import jax
import jax.numpy as jnp
from jax import lax
from jax.experimental import pallas as pl
from jax.experimental.pallas import tpu as pltpu
from jax.sharding import PartitionSpec as P

NORM_EPS = 1e-6
ROPE_THETA = 10000.0
F32 = jnp.float32
BF16 = jnp.bfloat16
SEQ_STEP = 4
FF_BLOCK = 512
VMEM_LIMIT = 67_043_328


def mm(a, b):
    return lax.dot_general(a, b, (((1,), (0,)), ((), ())), preferred_element_type=F32)


def mm_ta(a, b):
    return lax.dot_general(a, b, (((0,), (0,)), ((), ())), preferred_element_type=F32)


def mm_tb(a, b):
    return lax.dot_general(a, b, (((1,), (1,)), ((), ())), preferred_element_type=F32)


def partner_rows(x):
    rows, width = x.shape
    x3 = x.reshape(rows // 8, 8, width)
    odd = lax.broadcasted_iota(jnp.int32, x3.shape, 1) % 2 == 1
    return jnp.where(odd, pltpu.roll(x3, 1, 1), pltpu.roll(x3, 7, 1)).reshape(rows, width)


def rotate_rows(x, cos_t, sin_t, sign):
    rows, width = x.shape
    swapped = partner_rows(x)
    x3 = x.reshape(rows // 64, 64, width)
    s3 = swapped.reshape(rows // 64, 64, width)
    return (x3 * cos_t[None] + s3 * (sign * sin_t)[None]).reshape(rows, width)


def fold_lanes(x):
    out = x[:, :128]
    for j in range(1, x.shape[1] // 128):
        out = out + x[:, 128 * j:128 * (j + 1)]
    return out


ORDERS = ((1, 2, 4, 8, 16), (1, 4, 2, 8, 16), (1, 8, 16, 2, 4))
STEPS = 5
MATS = ((0, 1), (1, 1), (2, 1))
LANES = 512


def exchange_plan(ga_in, gf_in, ga_out, gf_out, acc_f, acc_a, rf0, rf1, rf2, rf3, rf4, ra0, ra1, ra2, ra3, ra4,
                    g_sum, g_got, in_sem, out_sem, rs_send, rs_recv, ag_send, ag_recv, g_in, g_send, g_recv):
    me = lax.axis_index("dp")
    bit = {b: lax.rem(lax.div(me, b), 2) for b in ORDERS[0]}
    mate = {b: me + b - 2 * b * bit[b] for b in ORDERS[0]}
    rf, ra = (rf0, rf1, rf2, rf3, rf4), (ra0, ra1, ra2, ra3, ra4)
    ff_rows, ga_rows = gf_in.shape[1], acc_a.shape[1] * 2
    segs = []
    for k in range(len(MATS) + 1):
        for color in range(3):
            if k < len(MATS):
                segs.append((k, color, True, MATS[k], len(segs)))
            elif color < 2:
                segs.append((k, color, False, None, len(segs)))

    def half(seg, s, mine, whole):
        _, color, is_f, _, _ = seg
        rows, lanes = (ff_rows, LANES) if is_f else (ga_rows, None)
        row, lane = 0, 0
        for t in range(s + 1):
            own = bit[ORDERS[color][t]]
            pick = own if (t < s or mine) else 1 - own
            if is_f and t >= 3:
                lanes //= 2
                lane = lane + pick * lanes
            else:
                rows //= 2
                if t > 0 or whole:
                    row = row + pick * rows
        return row, rows, lane, lanes

    def at(ref, seg, reg, whole):
        row, rows, lane, lanes = reg
        _, color, is_f, mats, _ = seg
        row = row if isinstance(row, int) else pl.multiple_of(row, 8)
        if is_f:
            if whole:
                lane = lane + color * LANES
            lane = lane if isinstance(lane, int) else pl.multiple_of(lane, 128)
            if whole:
                return ref.at[pl.ds(*mats), pl.ds(row, rows), pl.ds(lane, lanes)]
            return ref.at[pl.ds(*mats), color, pl.ds(row, rows), pl.ds(lane, lanes)]
        if whole:
            return ref.at[pl.ds(color * ga_rows + row, rows)]
        return ref.at[color, pl.ds(row, rows)]

    def got(seg, s):
        _, color, is_f, mats, _ = seg
        return rf[s].at[pl.ds(*mats), color] if is_f else ra[s].at[color]

    def acc_of(seg):
        return acc_f if seg[2] else acc_a

    def in_of(seg):
        return gf_in if seg[2] else ga_in

    def out_of(seg):
        return gf_out if seg[2] else ga_out

    def rs_copy(seg, s):
        if s == 0:
            src = at(in_of(seg), seg, half(seg, 0, False, True), True)
        else:
            src = at(acc_of(seg), seg, half(seg, s, False, False), False)
        return pltpu.make_async_remote_copy(src_ref=src, dst_ref=got(seg, s), send_sem=rs_send.at[seg[4], s],
                                            recv_sem=rs_recv.at[seg[4], s], device_id=(mate[ORDERS[seg[1]][s]],),
                                            device_id_type=pl.DeviceIdType.MESH)

    def ag_copy(seg, s):
        place = at(out_of(seg), seg, half(seg, s, True, True), True)
        src = at(acc_of(seg), seg, half(seg, s, True, False), False) if s == STEPS - 1 else place
        return pltpu.make_async_remote_copy(src_ref=src, dst_ref=place, send_sem=ag_send.at[seg[4], s],
                                            recv_sem=ag_recv.at[seg[4], s], device_id=(mate[ORDERS[seg[1]][s]],),
                                            device_id_type=pl.DeviceIdType.MESH)

    def load_own(seg):
        return pltpu.make_async_copy(at(in_of(seg), seg, half(seg, 0, True, True), True),
                                     acc_of(seg).at[pl.ds(*seg[3]), seg[1]] if seg[2] else acc_of(seg).at[seg[1]],
                                     in_sem.at[seg[4]])

    def store_own(seg):
        return pltpu.make_async_copy(at(acc_of(seg), seg, half(seg, STEPS - 1, True, False), False),
                                     at(out_of(seg), seg, half(seg, STEPS - 1, True, True), True), out_sem.at[seg[4]])

    def gain_copy(s):
        return pltpu.make_async_remote_copy(src_ref=g_sum.at[s], dst_ref=g_got.at[s], send_sem=g_send.at[s],
                                            recv_sem=g_recv.at[s], device_id=(mate[ORDERS[0][s]],),
                                            device_id_type=pl.DeviceIdType.MESH)

    gain_rows = pl.ds(2 * ga_rows, 8)

    def gain_in():
        return pltpu.make_async_copy(ga_in.at[gain_rows], g_sum.at[0], g_in.at[0])

    def gain_out():
        return pltpu.make_async_copy(g_sum.at[STEPS], ga_out.at[gain_rows], g_in.at[1])

    def begin():
        barrier = pltpu.get_barrier_semaphore()
        for b in ORDERS[0]:
            pl.semaphore_signal(barrier, inc=1, device_id=(mate[b],), device_id_type=pl.DeviceIdType.MESH)
        pl.semaphore_wait(barrier, STEPS)
        for seg in segs:
            rs_copy(seg, 0).start()
            load_own(seg).start()
        gain_in().start()
        gain_in().wait()
        gain_copy(0).start()

    def advance(seg, s):
        if 1 <= s <= STEPS:
            rs_copy(seg, s - 1).wait_recv()
            if s == 1:
                load_own(seg).wait()
            kept = at(acc_of(seg), seg, half(seg, s - 1, True, False), False)
            kept[...] = kept[...] + got(seg, s - 1)[...]
            if s < STEPS:
                rs_copy(seg, s).start()
            else:
                ag_copy(seg, STEPS - 1).start()
                store_own(seg).start()
        else:
            u = 2 * STEPS - s
            ag_copy(seg, u).wait_recv()
            if u == STEPS - 1:
                store_own(seg).wait()
            if u > 0:
                ag_copy(seg, u - 1).start()

    def wave(w):
        for seg in segs:
            s = w - seg[0]
            if 1 <= s <= 2 * STEPS:
                advance(seg, s)
        if w <= STEPS:
            gain_copy(w - 1).wait_recv()
            g_sum[w] = g_sum[w - 1] + g_got[w - 1]
            if w < STEPS:
                gain_copy(w).start()
            else:
                gain_out().start()

    def finish():
        for seg in segs:
            for s in range(STEPS):
                rs_copy(seg, s).wait_send()
                ag_copy(seg, s).wait_send()
        for s in range(STEPS):
            gain_copy(s).wait_send()
        gain_out().wait()

    return begin, wave, finish


WAVES = 2 * STEPS + len(MATS)


def exchange_kernel(*refs):
    begin, wave, finish = exchange_plan(*refs)
    begin()
    for w in range(1, WAVES + 1):
        wave(w)
    finish()


def exchange_scratch(ga, gf):
    half_rows, dim = (ga.shape[0] - 8) // 2, ga.shape[1]
    mats, ff_rows, _ = gf.shape
    n_seg = 3 * len(MATS) + 2
    f_sizes = [(ff_rows // 2, LANES), (ff_rows // 4, LANES), (ff_rows // 8, LANES), (ff_rows // 8, LANES // 2), (ff_rows // 8, LANES // 4)]
    dma = pltpu.SemaphoreType.DMA
    return ([pltpu.VMEM((mats, 3, ff_rows // 2, LANES), F32), pltpu.VMEM((2, half_rows // 2, dim), F32)]
            + [pltpu.VMEM((mats, 3) + size, F32) for size in f_sizes]
            + [pltpu.VMEM((2, half_rows >> (s + 1), dim), F32) for s in range(STEPS)]
            + [pltpu.VMEM((STEPS + 1, 8, dim), F32), pltpu.VMEM((STEPS, 8, dim), F32),
               dma((n_seg,)), dma((n_seg,)), dma((n_seg, STEPS)), dma((n_seg, STEPS)), dma((n_seg, STEPS)),
               dma((n_seg, STEPS)), dma((2,)), dma((STEPS,)), dma((STEPS,))])


def exchange(ga, gf):
    any_spec = pl.BlockSpec(memory_space=pl.ANY)
    return pl.pallas_call(
        exchange_kernel,
        out_shape=(jax.ShapeDtypeStruct(ga.shape, F32), jax.ShapeDtypeStruct(gf.shape, F32)),
        in_specs=[any_spec, any_spec],
        out_specs=(any_spec, any_spec),
        scratch_shapes=exchange_scratch(ga, gf),
        compiler_params=pltpu.CompilerParams(collective_id=0, has_side_effects=True, vmem_limit_bytes=VMEM_LIMIT),
        cost_estimate=pl.CostEstimate(flops=50_000_000_000, bytes_accessed=60_000_000, transcendentals=0),
    )(ga, gf)


def layer_body(beside, n_steps, n_heads, kv_heads, scale,
                 x_ref, d_ref, wqkv_ref, wo_ref, wg_ref, wu_ref, wd_ref, gains_ref, cos_ref, sin_ref,
                 dx_ref, ga_ref, gf_ref,
                 q_s, k_s, v_s, a_s, da_s, p_s, dqkv_s, dn2_s, gacc_s):
    step = pl.program_id(0)
    seqs = x_ref.shape[0]
    dim = x_ref.shape[1]
    hd = 64
    nq, nkv = n_heads * hd, kv_heads * hd
    grp = n_heads // kv_heads
    ff = wg_ref.shape[1]
    seq = x_ref.shape[2]

    @pl.when(step == 0)
    def _():
        ga_ref[...] = jnp.zeros_like(ga_ref)
        gf_ref[...] = jnp.zeros_like(gf_ref)
        gacc_s[...] = jnp.zeros_like(gacc_s)

    cos_t = cos_ref[...]
    sin_t = sin_ref[...]
    xb = jnp.concatenate([x_ref[b] for b in range(seqs)], axis=1)
    db = jnp.concatenate([d_ref[b] for b in range(seqs)], axis=1)
    xf = xb.astype(F32)
    g_attn = gains_ref[0]
    g_ffn = gains_ref[1]
    inv_a = lax.rsqrt(jnp.mean(xf * xf, axis=0, keepdims=True) + NORM_EPS)
    nb = (xf * inv_a * g_attn).astype(BF16)
    qkv = mm(wqkv_ref[...], nb)
    rot = rotate_rows(qkv[:nq + nkv].astype(BF16).astype(F32), cos_t, sin_t, 1.0).astype(BF16)
    q_s[...] = rot[:nq]
    k_s[...] = rot[nq:]
    v_s[...] = qkv[nq + nkv:].astype(BF16)

    t_idx = lax.broadcasted_iota(jnp.int32, (seq, grp * seq), 0)
    s_idx = lax.broadcasted_iota(jnp.int32, (seq, grp * seq), 1) % seq
    causal = s_idx >= t_idx

    def heads_of(ref, kv, lanes):
        return jnp.concatenate([ref[(kv * grp + g) * hd:(kv * grp + g + 1) * hd, lanes] for g in range(grp)], axis=1)

    for b in range(seqs):
        lanes = slice(b * seq, (b + 1) * seq)
        for kv in range(kv_heads):
            rows = slice(kv * hd, (kv + 1) * hd)
            sc = mm_ta(k_s[rows, lanes], heads_of(q_s, kv, lanes)) * scale
            sc = jnp.where(causal, sc, -1e30)
            ex = jnp.exp(sc - jnp.max(sc, axis=0, keepdims=True))
            p = ex / jnp.sum(ex, axis=0, keepdims=True)
            p_s[b * kv_heads + kv] = p
            a = mm(v_s[rows, lanes], p.astype(BF16)).astype(BF16)
            for g in range(grp):
                h = kv * grp + g
                a_s[h * hd:(h + 1) * hd, lanes] = a[:, g * seq:(g + 1) * seq]

    beside(step, 0)
    mb = (xf + mm_ta(wo_ref[...], a_s[...])).astype(BF16)
    mf = mb.astype(F32)
    inv_f = lax.rsqrt(jnp.mean(mf * mf, axis=0, keepdims=True) + NORM_EPS)
    n2 = (mf * inv_f * g_ffn).astype(BF16)

    for j in range(ff // FF_BLOCK):
        cols = slice(j * FF_BLOCK, (j + 1) * FF_BLOCK)
        gate = mm_ta(wg_ref[:, cols], n2).astype(BF16).astype(F32)
        up = mm_ta(wu_ref[:, cols], n2).astype(BF16).astype(F32)
        dh = mm_ta(wd_ref[:, cols], db).astype(BF16).astype(F32)
        sig = jax.nn.sigmoid(gate)
        silu = gate * sig
        hid = (silu * up).astype(BF16)
        dgate = (dh * up * sig * (1.0 + gate * (1.0 - sig))).astype(BF16)
        dup = (dh * silu).astype(BF16)
        gf_ref[0, :, cols] += mm_tb(n2, dgate)
        gf_ref[1, :, cols] += mm_tb(n2, dup)
        gf_ref[2, :, cols] += mm_tb(db, hid)
        part = mm(wg_ref[:, cols], dgate) + mm(wu_ref[:, cols], dup)
        if j == 0:
            dn2_s[...] = part
            beside(step, 1)
        else:
            dn2_s[...] += part

    beside(step, 2)

    dn2 = dn2_s[...].astype(BF16).astype(F32)
    sc2 = dn2 * g_ffn
    dmid = inv_f * sc2 - mf * (inv_f * inv_f * inv_f) * jnp.mean(sc2 * mf, axis=0, keepdims=True)
    gacc_s[1] += fold_lanes(dn2 * mf * inv_f)
    dmb = (db.astype(F32) + dmid).astype(BF16)
    ga_ref[nq + 2 * nkv:2 * nq + 2 * nkv, :] += mm_tb(a_s[...], dmb)
    da_s[...] = mm(wo_ref[...], dmb).astype(BF16)

    for b in range(seqs):
        lanes = slice(b * seq, (b + 1) * seq)
        for kv in range(kv_heads):
            rows = slice(kv * hd, (kv + 1) * hd)
            da = heads_of(da_s, kv, lanes)
            p = p_s[b * kv_heads + kv]
            dp = mm_ta(v_s[rows, lanes], da).astype(BF16).astype(F32)
            dqkv_s[nq + nkv + kv * hd:nq + nkv + (kv + 1) * hd, lanes] = mm_tb(da, p.astype(BF16))
            rd = jnp.sum(p * dp, axis=0, keepdims=True)
            ds = (p * (dp - rd) * scale).astype(BF16)
            dq = mm(k_s[rows, lanes], ds)
            for g in range(grp):
                h = kv * grp + g
                dqkv_s[h * hd:(h + 1) * hd, lanes] = dq[:, g * seq:(g + 1) * seq]
            dqkv_s[nq + kv * hd:nq + (kv + 1) * hd, lanes] = mm_tb(heads_of(q_s, kv, lanes), ds)

    beside(step, 3)
    drot = dqkv_s[:nq + nkv].astype(BF16).astype(F32)
    dqk = rotate_rows(drot, cos_t, sin_t, -1.0).astype(BF16)
    dqkv = jnp.concatenate([dqk, dqkv_s[nq + nkv:].astype(BF16)], axis=0)
    ga_ref[:nq + 2 * nkv, :] += mm_tb(dqkv, nb)
    dn = mm_ta(wqkv_ref[...], dqkv).astype(BF16).astype(F32)
    sc1 = dn * g_attn
    dxn = inv_a * sc1 - xf * (inv_a * inv_a * inv_a) * jnp.mean(sc1 * xf, axis=0, keepdims=True)
    gacc_s[0] += fold_lanes(dn * xf * inv_a)
    dx = (dmb.astype(F32) + dxn).astype(BF16)
    for b in range(seqs):
        dx_ref[b] = dx[:, b * seq:(b + 1) * seq]

    @pl.when(step == n_steps - 1)
    def _():
        ra = jnp.sum(jnp.transpose(gacc_s[0]), axis=0, keepdims=True)
        rf = jnp.sum(jnp.transpose(gacc_s[1]), axis=0, keepdims=True)
        row = lax.broadcasted_iota(jnp.int32, (8, dim), 0)
        ga_ref[2 * nq + 2 * nkv:, :] = jnp.where(row == 0, ra, jnp.where(row == 1, rf, 0.0))


def layer_kernel(n_steps, n_heads, kv_heads, scale, *refs):
    layer_body(lambda step, point: None, n_steps, n_heads, kv_heads, scale, *refs)


def layer_exchange_kernel(n_steps, n_heads, kv_heads, scale, *refs):
    ins, more_in, outs, more_out, rest = refs[:10], refs[10:12], refs[12:15], refs[15:17], refs[17:]
    begin, wave, finish = exchange_plan(*more_in, *more_out, *rest[N_SCRATCH:])

    @pl.when(pl.program_id(0) == 0)
    def _():
        begin()

    def beside(step, point):
        for i in range(n_steps):
            w = i * 4 + point + 1
            if w <= WAVES:
                @pl.when(step == i)
                def _():
                    wave(w)

    layer_body(beside, n_steps, n_heads, kv_heads, scale, *ins, *outs, *rest[:N_SCRATCH])

    @pl.when(pl.program_id(0) == n_steps - 1)
    def _():
        for w in range(n_steps * 4 + 1, WAVES + 1):
            wave(w)
        finish()


N_SCRATCH = 9


def layer_call(x_t, d_t, wqkv, wo, wg, wu, wd, gains, cos_t, sin_t, n_heads, kv_heads, others=()):
    n_seq, dim, seq = x_t.shape
    hd = 64
    nq, nkv = n_heads * hd, kv_heads * hd
    ff = wg.shape[1]
    width = SEQ_STEP * seq
    n_steps = n_seq // SEQ_STEP
    tok = n_seq * seq
    once = pl.Buffered(buffer_count=1)
    any_spec = pl.BlockSpec(memory_space=pl.ANY)

    def whole(shape):
        return pl.BlockSpec(shape, lambda i: (0,) * len(shape), pipeline_mode=once)

    act = pl.BlockSpec((SEQ_STEP, dim, seq), lambda i: (i, 0, 0))
    ga_rows = 2 * nq + 2 * nkv + 8
    extra = {}
    scratch = [
        pltpu.VMEM((nq, width), BF16), pltpu.VMEM((nkv, width), BF16), pltpu.VMEM((nkv, width), BF16),
        pltpu.VMEM((nq, width), BF16), pltpu.VMEM((nq, width), BF16),
        pltpu.VMEM((SEQ_STEP * kv_heads, seq, (n_heads // kv_heads) * seq), F32),
        pltpu.VMEM((nq + 2 * nkv, width), F32), pltpu.VMEM((dim, width), F32), pltpu.VMEM((2, dim, 128), F32)]
    body = layer_kernel
    if others:
        extra = dict(collective_id=1, has_side_effects=True)
        scratch += exchange_scratch(*others)
        body = layer_exchange_kernel
    return pl.pallas_call(
        functools.partial(body, n_steps, n_heads, kv_heads, hd ** -0.5),
        grid=(n_steps,),
        out_shape=(jax.ShapeDtypeStruct(x_t.shape, BF16),
                   jax.ShapeDtypeStruct((ga_rows, dim), F32),
                   jax.ShapeDtypeStruct((3, dim, ff), F32)) + tuple(jax.ShapeDtypeStruct(o.shape, F32) for o in others),
        in_specs=[act, act, whole(wqkv.shape), whole(wo.shape), whole(wg.shape), whole(wu.shape), whole(wd.shape),
                  whole(gains.shape), whole(cos_t.shape), whole(sin_t.shape)] + [any_spec] * len(others),
        out_specs=(act, whole((ga_rows, dim)), whole((3, dim, ff))) + (any_spec,) * len(others),
        scratch_shapes=scratch,
        compiler_params=pltpu.CompilerParams(dimension_semantics=("arbitrary",), vmem_limit_bytes=VMEM_LIMIT, **extra),
        cost_estimate=pl.CostEstimate(flops=2 * tok * 11 * dim * ff, bytes_accessed=40_000_000, transcendentals=0),
    )(x_t, d_t, wqkv, wo, wg, wu, wd, gains, cos_t, sin_t, *others)


def rope_rows(seq, hd):
    positions = jnp.arange(seq, dtype=F32)
    inv_freq = ROPE_THETA ** (-jnp.arange(0, hd, 2, dtype=F32) / hd)
    angles = positions[:, None] * inv_freq[None, :]
    cos_t = jnp.repeat(jnp.cos(angles).T, 2, axis=0)
    sin_h = jnp.sin(angles).T
    sin_t = jnp.stack([-sin_h, sin_h], axis=1).reshape(hd, seq)
    return jnp.tile(cos_t, (1, SEQ_STEP)), jnp.tile(sin_t, (1, SEQ_STEP))


def layers(x_layer0, x_layer1, d_out, g_attn, w_q, w_k, w_v, w_o, g_ffn, w_gate, w_up, w_down):
    dim, n_heads, kv_heads, hd = w_q.shape[1], w_q.shape[2], w_k.shape[2], w_q.shape[3]
    cos_t, sin_t = rope_rows(x_layer0.shape[1], hd)

    def flat(w):
        return w.transpose(0, 2, 3, 1).reshape(2, -1, dim)

    wqkv = jnp.concatenate([flat(w_q), flat(w_k), flat(w_v)], axis=1)
    wo = w_o.reshape(2, n_heads * hd, dim)
    wd = w_down.transpose(0, 2, 1)
    gains = jnp.stack([g_attn, g_ffn], axis=1).astype(F32)[..., None]

    def run(layer, x, d_t, others=()):
        return layer_call(x.transpose(0, 2, 1), d_t, wqkv[layer], wo[layer], w_gate[layer], w_up[layer], wd[layer],
                          gains[layer], cos_t, sin_t, n_heads, kv_heads, others)

    d1, ga1, gf1 = run(1, x_layer1, d_out.transpose(0, 2, 1))
    d0, ga0, gf0, ga1, gf1 = run(0, x_layer0, d1, (ga1, gf1))
    return d0, exchange(ga0, gf0), (ga1, gf1)


def solution(mesh):
    num_devices = mesh.shape["dp"]
    act_spec = P("dp", None, None)
    rep_spec = P()

    def local_step(*args):
        w_q, w_k = args[4], args[5]
        dim, n_heads, kv_heads, hd = w_q.shape[1], w_q.shape[2], w_k.shape[2], w_q.shape[3]
        nq, nkv = n_heads * hd, kv_heads * hd
        d0, low, top = layers(*args)
        ga = jnp.stack([low[0], top[0]]) * (1.0 / num_devices)
        gf = jnp.stack([low[1], top[1]]) * (1.0 / num_devices)

        def heads(rows):
            return rows.reshape(2, -1, hd, dim).transpose(0, 3, 1, 2)

        o_at = nq + 2 * nkv
        return (d0.transpose(0, 2, 1), ga[:, o_at + nq], heads(ga[:, :nq]), heads(ga[:, nq:nq + nkv]),
                heads(ga[:, nq + nkv:o_at]), ga[:, o_at:o_at + nq].reshape(2, n_heads, hd, dim), ga[:, o_at + nq + 1],
                gf[:, 0], gf[:, 1], gf[:, 2].transpose(0, 2, 1))

    return jax.shard_map(local_step, mesh=mesh, in_specs=(act_spec,) * 3 + (rep_spec,) * 9, out_specs=(act_spec,) + (rep_spec,) * 9, check_vma=False)
```

```python
import functools

import jax
import jax.numpy as jnp
from jax import lax
from jax.experimental import pallas as pl
from jax.experimental.pallas import tpu as pltpu
from jax.sharding import PartitionSpec as P

NORM_EPS = 1e-6
ROPE_THETA = 10000.0
F32 = jnp.float32
BF16 = jnp.bfloat16
SEQ_STEP = 4
FF_BLOCK = 512
VMEM_LIMIT = 67_043_328


def mm(a, b):
    return lax.dot_general(a, b, (((1,), (0,)), ((), ())), preferred_element_type=F32)


def mm_ta(a, b):
    return lax.dot_general(a, b, (((0,), (0,)), ((), ())), preferred_element_type=F32)


def mm_tb(a, b):
    return lax.dot_general(a, b, (((1,), (1,)), ((), ())), preferred_element_type=F32)


def partner_rows(x):
    rows, width = x.shape
    x3 = x.reshape(rows // 8, 8, width)
    odd = lax.broadcasted_iota(jnp.int32, x3.shape, 1) % 2 == 1
    return jnp.where(odd, pltpu.roll(x3, 1, 1), pltpu.roll(x3, 7, 1)).reshape(rows, width)


def rotate_rows(x, cos_t, sin_t, sign):
    rows, width = x.shape
    swapped = partner_rows(x)
    x3 = x.reshape(rows // 64, 64, width)
    s3 = swapped.reshape(rows // 64, 64, width)
    return (x3 * cos_t[None] + s3 * (sign * sin_t)[None]).reshape(rows, width)


def fold_lanes(x):
    out = x[:, :128]
    for j in range(1, x.shape[1] // 128):
        out = out + x[:, 128 * j:128 * (j + 1)]
    return out


ORDERS = ((1, 2, 4, 8, 16), (1, 4, 2, 8, 16), (1, 8, 16, 2, 4))
STEPS = 5
MATS = ((0, 1), (1, 1), (2, 1))
LANES = 512


def exchange_plan(ga_in, gf_in, ga_out, gf_out, acc_f, acc_a, rf0, rf1, rf2, rf3, rf4, ra0, ra1, ra2, ra3, ra4,
                    g_sum, g_got, in_sem, out_sem, rs_send, rs_recv, ag_send, ag_recv, g_in, g_send, g_recv):
    me = lax.axis_index("dp")
    bit = {b: lax.rem(lax.div(me, b), 2) for b in ORDERS[0]}
    mate = {b: me + b - 2 * b * bit[b] for b in ORDERS[0]}
    rf, ra = (rf0, rf1, rf2, rf3, rf4), (ra0, ra1, ra2, ra3, ra4)
    ff_rows, ga_rows = gf_in.shape[1], acc_a.shape[1] * 2
    segs = []
    for k in range(len(MATS) + 1):
        for color in range(3):
            if k < len(MATS):
                segs.append((k, color, True, MATS[k], len(segs)))
            elif color < 2:
                segs.append((k, color, False, None, len(segs)))

    def half(seg, s, mine, whole):
        _, color, is_f, _, _ = seg
        rows, lanes = (ff_rows, LANES) if is_f else (ga_rows, None)
        row, lane = 0, 0
        for t in range(s + 1):
            own = bit[ORDERS[color][t]]
            pick = own if (t < s or mine) else 1 - own
            if is_f and t >= 3:
                lanes //= 2
                lane = lane + pick * lanes
            else:
                rows //= 2
                if t > 0 or whole:
                    row = row + pick * rows
        return row, rows, lane, lanes

    def at(ref, seg, reg, whole):
        row, rows, lane, lanes = reg
        _, color, is_f, mats, _ = seg
        row = row if isinstance(row, int) else pl.multiple_of(row, 8)
        if is_f:
            if whole:
                lane = lane + color * LANES
            lane = lane if isinstance(lane, int) else pl.multiple_of(lane, 128)
            if whole:
                return ref.at[pl.ds(*mats), pl.ds(row, rows), pl.ds(lane, lanes)]
            return ref.at[pl.ds(*mats), color, pl.ds(row, rows), pl.ds(lane, lanes)]
        if whole:
            return ref.at[pl.ds(color * ga_rows + row, rows)]
        return ref.at[color, pl.ds(row, rows)]

    def got(seg, s):
        _, color, is_f, mats, _ = seg
        return rf[s].at[pl.ds(*mats), color] if is_f else ra[s].at[color]

    def acc_of(seg):
        return acc_f if seg[2] else acc_a

    def in_of(seg):
        return gf_in if seg[2] else ga_in

    def out_of(seg):
        return gf_out if seg[2] else ga_out

    def rs_copy(seg, s):
        if s == 0:
            src = at(in_of(seg), seg, half(seg, 0, False, True), True)
        else:
            src = at(acc_of(seg), seg, half(seg, s, False, False), False)
        return pltpu.make_async_remote_copy(src_ref=src, dst_ref=got(seg, s), send_sem=rs_send.at[seg[4], s],
                                            recv_sem=rs_recv.at[seg[4], s], device_id=(mate[ORDERS[seg[1]][s]],),
                                            device_id_type=pl.DeviceIdType.MESH)

    def ag_copy(seg, s):
        place = at(out_of(seg), seg, half(seg, s, True, True), True)
        src = at(acc_of(seg), seg, half(seg, s, True, False), False) if s == STEPS - 1 else place
        return pltpu.make_async_remote_copy(src_ref=src, dst_ref=place, send_sem=ag_send.at[seg[4], s],
                                            recv_sem=ag_recv.at[seg[4], s], device_id=(mate[ORDERS[seg[1]][s]],),
                                            device_id_type=pl.DeviceIdType.MESH)

    def load_own(seg):
        return pltpu.make_async_copy(at(in_of(seg), seg, half(seg, 0, True, True), True),
                                     acc_of(seg).at[pl.ds(*seg[3]), seg[1]] if seg[2] else acc_of(seg).at[seg[1]],
                                     in_sem.at[seg[4]])

    def store_own(seg):
        return pltpu.make_async_copy(at(acc_of(seg), seg, half(seg, STEPS - 1, True, False), False),
                                     at(out_of(seg), seg, half(seg, STEPS - 1, True, True), True), out_sem.at[seg[4]])

    def gain_copy(s):
        return pltpu.make_async_remote_copy(src_ref=g_sum.at[s], dst_ref=g_got.at[s], send_sem=g_send.at[s],
                                            recv_sem=g_recv.at[s], device_id=(mate[ORDERS[0][s]],),
                                            device_id_type=pl.DeviceIdType.MESH)

    gain_rows = pl.ds(2 * ga_rows, 8)

    def gain_in():
        return pltpu.make_async_copy(ga_in.at[gain_rows], g_sum.at[0], g_in.at[0])

    def gain_out():
        return pltpu.make_async_copy(g_sum.at[STEPS], ga_out.at[gain_rows], g_in.at[1])

    def begin():
        barrier = pltpu.get_barrier_semaphore()
        for b in ORDERS[0]:
            pl.semaphore_signal(barrier, inc=1, device_id=(mate[b],), device_id_type=pl.DeviceIdType.MESH)
        pl.semaphore_wait(barrier, STEPS)
        for seg in segs:
            rs_copy(seg, 0).start()
            load_own(seg).start()
        gain_in().start()
        gain_in().wait()
        gain_copy(0).start()

    def advance(seg, s):
        if 1 <= s <= STEPS:
            rs_copy(seg, s - 1).wait_recv()
            if s == 1:
                load_own(seg).wait()
            kept = at(acc_of(seg), seg, half(seg, s - 1, True, False), False)
            kept[...] = kept[...] + got(seg, s - 1)[...]
            if s < STEPS:
                rs_copy(seg, s).start()
            else:
                ag_copy(seg, STEPS - 1).start()
                store_own(seg).start()
        else:
            u = 2 * STEPS - s
            ag_copy(seg, u).wait_recv()
            if u == STEPS - 1:
                store_own(seg).wait()
            if u > 0:
                ag_copy(seg, u - 1).start()

    def wave(w):
        for seg in segs:
            s = w - seg[0]
            if 1 <= s <= 2 * STEPS:
                advance(seg, s)
        if w <= STEPS:
            gain_copy(w - 1).wait_recv()
            g_sum[w] = g_sum[w - 1] + g_got[w - 1]
            if w < STEPS:
                gain_copy(w).start()
            else:
                gain_out().start()

    def finish():
        for seg in segs:
            for s in range(STEPS):
                rs_copy(seg, s).wait_send()
                ag_copy(seg, s).wait_send()
        for s in range(STEPS):
            gain_copy(s).wait_send()
        gain_out().wait()

    return begin, wave, finish


WAVES = 2 * STEPS + len(MATS)
SLOT_WAVE = {0: 1, 1: 2, 3: 3, 5: 4, 7: 5, 8: 6, 9: 7, 10: 8, 11: 9, 12: 10, 14: 11, 15: 12}


def exchange_kernel(*refs):
    begin, wave, finish = exchange_plan(*refs)
    begin()
    for w in range(1, WAVES + 1):
        wave(w)
    finish()


def exchange_scratch(ga, gf):
    half_rows, dim = (ga.shape[0] - 8) // 2, ga.shape[1]
    mats, ff_rows, _ = gf.shape
    n_seg = 3 * len(MATS) + 2
    f_sizes = [(ff_rows // 2, LANES), (ff_rows // 4, LANES), (ff_rows // 8, LANES), (ff_rows // 8, LANES // 2), (ff_rows // 8, LANES // 4)]
    dma = pltpu.SemaphoreType.DMA
    return ([pltpu.VMEM((mats, 3, ff_rows // 2, LANES), F32), pltpu.VMEM((2, half_rows // 2, dim), F32)]
            + [pltpu.VMEM((mats, 3) + size, F32) for size in f_sizes]
            + [pltpu.VMEM((2, half_rows >> (s + 1), dim), F32) for s in range(STEPS)]
            + [pltpu.VMEM((STEPS + 1, 8, dim), F32), pltpu.VMEM((STEPS, 8, dim), F32),
               dma((n_seg,)), dma((n_seg,)), dma((n_seg, STEPS)), dma((n_seg, STEPS)), dma((n_seg, STEPS)),
               dma((n_seg, STEPS)), dma((2,)), dma((STEPS,)), dma((STEPS,))])


def exchange(ga, gf):
    any_spec = pl.BlockSpec(memory_space=pl.ANY)
    return pl.pallas_call(
        exchange_kernel,
        out_shape=(jax.ShapeDtypeStruct(ga.shape, F32), jax.ShapeDtypeStruct(gf.shape, F32)),
        in_specs=[any_spec, any_spec],
        out_specs=(any_spec, any_spec),
        scratch_shapes=exchange_scratch(ga, gf),
        compiler_params=pltpu.CompilerParams(collective_id=0, has_side_effects=True, vmem_limit_bytes=VMEM_LIMIT),
        cost_estimate=pl.CostEstimate(flops=50_000_000_000, bytes_accessed=60_000_000, transcendentals=0),
    )(ga, gf)


def layer_body(beside, n_steps, n_heads, kv_heads, scale,
                 x_ref, d_ref, wq_ref, wk_ref, wv_ref, wo_ref, wg_ref, wu_ref, wd_ref, gains_ref, cos_ref, sin_ref,
                 dx_ref, ga_ref, gf_ref,
                 q_s, k_s, v_s, a_s, da_s, p_s, dqkv_s, dn2_s, gacc_s, wqkv_ref):
    step = pl.program_id(0)
    seqs = x_ref.shape[0]
    dim = x_ref.shape[1]
    hd = 64
    nq, nkv = n_heads * hd, kv_heads * hd
    grp = n_heads // kv_heads
    ff = wg_ref.shape[1]
    seq = x_ref.shape[2]

    @pl.when(step == 0)
    def _():
        ga_ref[...] = jnp.zeros_like(ga_ref)
        gf_ref[...] = jnp.zeros_like(gf_ref)
        gacc_s[...] = jnp.zeros_like(gacc_s)
        wqkv_ref[:nq] = wq_ref[...]
        wqkv_ref[nq:nq + nkv] = wk_ref[...]
        wqkv_ref[nq + nkv:] = wv_ref[...]

    cos_t = cos_ref[...]
    sin_t = sin_ref[...]
    xb = jnp.concatenate([x_ref[b] for b in range(seqs)], axis=1)
    db = jnp.concatenate([d_ref[b] for b in range(seqs)], axis=1)
    xf = xb.astype(F32)
    g_attn = gains_ref[0]
    g_ffn = gains_ref[1]
    inv_a = lax.rsqrt(jnp.mean(xf * xf, axis=0, keepdims=True) + NORM_EPS)
    nb = (xf * inv_a * g_attn).astype(BF16)
    qkv = mm(wqkv_ref[...], nb)
    rot = rotate_rows(qkv[:nq + nkv].astype(BF16).astype(F32), cos_t, sin_t, 1.0).astype(BF16)
    q_s[...] = rot[:nq]
    k_s[...] = rot[nq:]
    v_s[...] = qkv[nq + nkv:].astype(BF16)

    t_idx = lax.broadcasted_iota(jnp.int32, (seq, grp * seq), 0)
    s_idx = lax.broadcasted_iota(jnp.int32, (seq, grp * seq), 1) % seq
    causal = s_idx >= t_idx

    def heads_of(ref, kv, lanes):
        return jnp.concatenate([ref[(kv * grp + g) * hd:(kv * grp + g + 1) * hd, lanes] for g in range(grp)], axis=1)

    for b in range(seqs):
        lanes = slice(b * seq, (b + 1) * seq)
        for kv in range(kv_heads):
            rows = slice(kv * hd, (kv + 1) * hd)
            sc = mm_ta(k_s[rows, lanes], heads_of(q_s, kv, lanes)) * scale
            sc = jnp.where(causal, sc, -1e30)
            ex = jnp.exp(sc - jnp.max(sc, axis=0, keepdims=True))
            p = ex / jnp.sum(ex, axis=0, keepdims=True)
            p_s[b * kv_heads + kv] = p
            a = mm(v_s[rows, lanes], p.astype(BF16)).astype(BF16)
            for g in range(grp):
                h = kv * grp + g
                a_s[h * hd:(h + 1) * hd, lanes] = a[:, g * seq:(g + 1) * seq]

    beside(step, 0)
    mb = (xf + mm_ta(wo_ref[...], a_s[...])).astype(BF16)
    mf = mb.astype(F32)
    inv_f = lax.rsqrt(jnp.mean(mf * mf, axis=0, keepdims=True) + NORM_EPS)
    n2 = (mf * inv_f * g_ffn).astype(BF16)

    for j in range(ff // FF_BLOCK):
        cols = slice(j * FF_BLOCK, (j + 1) * FF_BLOCK)
        gate = mm_ta(wg_ref[:, cols], n2).astype(BF16).astype(F32)
        up = mm_ta(wu_ref[:, cols], n2).astype(BF16).astype(F32)
        dh = mm_ta(wd_ref[:, cols], db).astype(BF16).astype(F32)
        sig = jax.nn.sigmoid(gate)
        silu = gate * sig
        hid = (silu * up).astype(BF16)
        dgate = (dh * up * sig * (1.0 + gate * (1.0 - sig))).astype(BF16)
        dup = (dh * silu).astype(BF16)
        gf_ref[0, :, cols] += mm_tb(n2, dgate)
        gf_ref[1, :, cols] += mm_tb(n2, dup)
        gf_ref[2, :, cols] += mm_tb(db, hid)
        part = mm(wg_ref[:, cols], dgate) + mm(wu_ref[:, cols], dup)
        if j == 0:
            dn2_s[...] = part
            beside(step, 1)
        else:
            dn2_s[...] += part

    beside(step, 2)

    dn2 = dn2_s[...].astype(BF16).astype(F32)
    sc2 = dn2 * g_ffn
    dmid = inv_f * sc2 - mf * (inv_f * inv_f * inv_f) * jnp.mean(sc2 * mf, axis=0, keepdims=True)
    gacc_s[1] += fold_lanes(dn2 * mf * inv_f)
    dmb = (db.astype(F32) + dmid).astype(BF16)
    ga_ref[nq + 2 * nkv:2 * nq + 2 * nkv, :] += mm_tb(a_s[...], dmb)
    da_s[...] = mm(wo_ref[...], dmb).astype(BF16)

    for b in range(seqs):
        lanes = slice(b * seq, (b + 1) * seq)
        for kv in range(kv_heads):
            rows = slice(kv * hd, (kv + 1) * hd)
            da = heads_of(da_s, kv, lanes)
            p = p_s[b * kv_heads + kv]
            dp = mm_ta(v_s[rows, lanes], da).astype(BF16).astype(F32)
            dqkv_s[nq + nkv + kv * hd:nq + nkv + (kv + 1) * hd, lanes] = mm_tb(da, p.astype(BF16))
            rd = jnp.sum(p * dp, axis=0, keepdims=True)
            ds = (p * (dp - rd) * scale).astype(BF16)
            dq = mm(k_s[rows, lanes], ds)
            for g in range(grp):
                h = kv * grp + g
                dqkv_s[h * hd:(h + 1) * hd, lanes] = dq[:, g * seq:(g + 1) * seq]
            dqkv_s[nq + kv * hd:nq + (kv + 1) * hd, lanes] = mm_tb(heads_of(q_s, kv, lanes), ds)

    beside(step, 3)
    drot = dqkv_s[:nq + nkv].astype(BF16).astype(F32)
    dqk = rotate_rows(drot, cos_t, sin_t, -1.0).astype(BF16)
    dqkv = jnp.concatenate([dqk, dqkv_s[nq + nkv:].astype(BF16)], axis=0)
    ga_ref[:nq + 2 * nkv, :] += mm_tb(dqkv, nb)
    dn = mm_ta(wqkv_ref[...], dqkv).astype(BF16).astype(F32)
    sc1 = dn * g_attn
    dxn = inv_a * sc1 - xf * (inv_a * inv_a * inv_a) * jnp.mean(sc1 * xf, axis=0, keepdims=True)
    gacc_s[0] += fold_lanes(dn * xf * inv_a)
    dx = (dmb.astype(F32) + dxn).astype(BF16)
    for b in range(seqs):
        dx_ref[b] = dx[:, b * seq:(b + 1) * seq]

    @pl.when(step == n_steps - 1)
    def _():
        ra = jnp.sum(jnp.transpose(gacc_s[0]), axis=0, keepdims=True)
        rf = jnp.sum(jnp.transpose(gacc_s[1]), axis=0, keepdims=True)
        row = lax.broadcasted_iota(jnp.int32, (8, dim), 0)
        ga_ref[2 * nq + 2 * nkv:, :] = jnp.where(row == 0, ra, jnp.where(row == 1, rf, 0.0))


def layer_kernel(n_steps, n_heads, kv_heads, scale, *refs):
    layer_body(lambda step, point: None, n_steps, n_heads, kv_heads, scale, *refs)


def layer_exchange_kernel(n_steps, n_heads, kv_heads, scale, *refs):
    ins, more_in, outs, more_out, rest = refs[:12], refs[12:14], refs[14:17], refs[17:19], refs[19:]
    begin, wave, finish = exchange_plan(*more_in, *more_out, *rest[N_SCRATCH:])

    @pl.when(pl.program_id(0) == 0)
    def _():
        begin()

    def beside(step, point):
        for i in range(n_steps):
            w = SLOT_WAVE.get(i * 4 + point)
            if w is not None:
                @pl.when(step == i)
                def _(w=w):
                    wave(w)

    layer_body(beside, n_steps, n_heads, kv_heads, scale, *ins, *outs, *rest[:N_SCRATCH])

    @pl.when(pl.program_id(0) == n_steps - 1)
    def _():
        for w in range(max(SLOT_WAVE.values()) + 1, WAVES + 1):
            wave(w)
        finish()


N_SCRATCH = 10


def layer_call(layer, x_t, d_t, weights, gains, cos_t, sin_t, n_heads, kv_heads, others=()):
    n_seq, dim, seq = x_t.shape
    hd = 64
    nq, nkv = n_heads * hd, kv_heads * hd
    ff = weights[-1].shape[2]
    width = SEQ_STEP * seq
    n_steps = n_seq // SEQ_STEP
    tok = n_seq * seq
    once = pl.Buffered(buffer_count=1)
    any_spec = pl.BlockSpec(memory_space=pl.ANY)

    def whole(shape):
        return pl.BlockSpec(shape, lambda i: (0,) * len(shape), pipeline_mode=once)

    def picked(shape):
        return pl.BlockSpec((None,) + shape[1:], lambda i: (layer,) + (0,) * (len(shape) - 1), pipeline_mode=once)

    act = pl.BlockSpec((SEQ_STEP, dim, seq), lambda i: (i, 0, 0))
    ga_rows = 2 * nq + 2 * nkv + 8
    extra = {}
    scratch = [
        pltpu.VMEM((nq, width), BF16), pltpu.VMEM((nkv, width), BF16), pltpu.VMEM((nkv, width), BF16),
        pltpu.VMEM((nq, width), BF16), pltpu.VMEM((nq, width), BF16),
        pltpu.VMEM((SEQ_STEP * kv_heads, seq, (n_heads // kv_heads) * seq), F32),
        pltpu.VMEM((nq + 2 * nkv, width), F32), pltpu.VMEM((dim, width), F32), pltpu.VMEM((2, dim, 128), F32), pltpu.VMEM((nq + 2 * nkv, dim), BF16)]
    body = layer_kernel
    if others:
        extra = dict(collective_id=1, has_side_effects=True)
        scratch += exchange_scratch(*others)
        body = layer_exchange_kernel
    return pl.pallas_call(
        functools.partial(body, n_steps, n_heads, kv_heads, hd ** -0.5),
        grid=(n_steps,),
        out_shape=(jax.ShapeDtypeStruct(x_t.shape, BF16),
                   jax.ShapeDtypeStruct((ga_rows, dim), F32),
                   jax.ShapeDtypeStruct((3, dim, ff), F32)) + tuple(jax.ShapeDtypeStruct(o.shape, F32) for o in others),
        in_specs=[act, act] + [picked(w.shape) for w in weights] + [picked(gains.shape), whole(cos_t.shape), whole(sin_t.shape)] + [any_spec] * len(others),
        out_specs=(act, whole((ga_rows, dim)), whole((3, dim, ff))) + (any_spec,) * len(others),
        scratch_shapes=scratch,
        compiler_params=pltpu.CompilerParams(dimension_semantics=("arbitrary",), vmem_limit_bytes=VMEM_LIMIT, **extra),
        cost_estimate=pl.CostEstimate(flops=2 * tok * 11 * dim * ff, bytes_accessed=40_000_000, transcendentals=0),
    )(x_t, d_t, *weights, gains, cos_t, sin_t, *others)


def rope_rows(seq, hd):
    positions = jnp.arange(seq, dtype=F32)
    inv_freq = ROPE_THETA ** (-jnp.arange(0, hd, 2, dtype=F32) / hd)
    angles = positions[:, None] * inv_freq[None, :]
    cos_t = jnp.repeat(jnp.cos(angles).T, 2, axis=0)
    sin_h = jnp.sin(angles).T
    sin_t = jnp.stack([-sin_h, sin_h], axis=1).reshape(hd, seq)
    return jnp.tile(cos_t, (1, SEQ_STEP)), jnp.tile(sin_t, (1, SEQ_STEP))


def layers(x_layer0, x_layer1, d_out, g_attn, w_q, w_k, w_v, w_o, g_ffn, w_gate, w_up, w_down, talk=True):
    dim, n_heads, kv_heads, hd = w_q.shape[1], w_q.shape[2], w_k.shape[2], w_q.shape[3]
    cos_t, sin_t = rope_rows(x_layer0.shape[1], hd)

    def flat(w):
        return w.transpose(0, 2, 3, 1).reshape(2, -1, dim)

    weights = (flat(w_q), flat(w_k), flat(w_v), w_o.reshape(2, n_heads * hd, dim), w_gate, w_up, w_down.transpose(0, 2, 1))
    gains = jnp.stack([g_attn, g_ffn], axis=1).astype(F32)[..., None]

    def run(layer, x, d_t, others=()):
        return layer_call(layer, x.transpose(0, 2, 1), d_t, weights, gains, cos_t, sin_t, n_heads, kv_heads, others)

    d1, ga1, gf1 = run(1, x_layer1, d_out.transpose(0, 2, 1))
    if not talk:
        d0, ga0, gf0 = run(0, x_layer0, d1)
        return d0, (ga0, gf0), (ga1, gf1)
    d0, ga0, gf0, ga1, gf1 = run(0, x_layer0, d1, (ga1, gf1))
    return d0, exchange(ga0, gf0), (ga1, gf1)


def solution(mesh):
    num_devices = mesh.shape["dp"]
    act_spec = P("dp", None, None)
    rep_spec = P()

    def local_step(*args):
        w_q, w_k = args[4], args[5]
        dim, n_heads, kv_heads, hd = w_q.shape[1], w_q.shape[2], w_k.shape[2], w_q.shape[3]
        nq, nkv = n_heads * hd, kv_heads * hd
        d0, low, top = layers(*args)
        inv_count = 1.0 / num_devices

        def both(pick):
            return jnp.stack([pick(*low) * inv_count, pick(*top) * inv_count])

        def heads(start, stop):
            return both(lambda ga, gf: ga[start:stop]).reshape(2, -1, hd, dim).transpose(0, 3, 1, 2)

        o_at = nq + 2 * nkv
        return (d0.transpose(0, 2, 1), both(lambda ga, gf: ga[o_at + nq]), heads(0, nq), heads(nq, nq + nkv),
                heads(nq + nkv, o_at), both(lambda ga, gf: ga[o_at:o_at + nq]).reshape(2, n_heads, hd, dim),
                both(lambda ga, gf: ga[o_at + nq + 1]), both(lambda ga, gf: gf[0]), both(lambda ga, gf: gf[1]),
                both(lambda ga, gf: gf[2]).transpose(0, 2, 1))

    return jax.shard_map(local_step, mesh=mesh, in_specs=(act_spec,) * 3 + (rep_spec,) * 9, out_specs=(act_spec,) + (rep_spec,) * 9, check_vma=False)
```
